128 devices in a mesh: section: 8 (over z, core), tp: 16 (over x, y).
Axes of the slice: x: 4, y: 4, z: 4, core: 2. Of those that a mesh axis runs over, the one named last changes fastest.
Arguments:
- latents: bfloat16 [1024, 16, 2048], P('tp', 'section'), may hold values from -6 to 6
- timestep: int32 [16], replicated, may hold values from 0 to 999
- target: int32 [16], replicated, may hold values from 0 to 7, as said below
- qkv_weight: bfloat16 [8, 2048, 3, 2048], P('section', None, None, 'tp'), may hold values from -0.125 to 0.125
- mod_weight: bfloat16 [8, 256, 3, 2048], P('section'), may hold values from -2.6 to 2.6
- out_weight: bfloat16 [8, 2048, 2048], P('section', 'tp'), may hold values from -0.125 to 0.125
Outputs:
- updated: bfloat16 [1024, 16, 2048], P('tp', 'section')
The draws below stay inside these ranges and needn't reach their ends.
Inputs may be any that keep to these rules, and one draw needn't show every extreme that they name: target[l] is l // 2 or l // 2 + 1; of one section's 2 latents at most 1 name the next section, exactly 1 for section 0, none for the last section.
All inputs are finite; a program needn't handle non-finite values.
Results may differ from the reference program's by a relative error of at most 0.023.
Values may be sent and summed in bfloat16 or wider, within the bound.
A program may use at most 128 MiB of HBM per device.

```python
import math
import jax
import jax.numpy as jnp
from jax import lax

D = 2048
HEADS = 16
HEAD_DIM = 128
FREQ = 256
TOK = 1024
LAT_SECTION = 2
MOVE_MAX = 1
SECTIONS = 8
LATENTS = 16
N_TP = 16


def draw_target(key, part):
    counts = jax.random.randint(jax.random.fold_in(key, 11), (SECTIONS,), 0, MOVE_MAX + 1)
    section_ids = jnp.arange(SECTIONS, dtype=jnp.int32)
    counts = jnp.where(section_ids == 0, MOVE_MAX, counts)
    counts = jnp.where(section_ids == SECTIONS - 1, 0, counts)
    row_keys = jax.random.split(jax.random.fold_in(key, 12), SECTIONS)
    ranks = jax.vmap(lambda row_key: jax.random.permutation(row_key, LAT_SECTION))(row_keys)
    movers = (ranks < counts[:, None]).astype(jnp.int32)
    return (section_ids[:, None] + movers).reshape(LATENTS).astype(jnp.int32)


def draw_mod_weight(key, part):
    base = jnp.clip(jax.random.normal(jax.random.fold_in(key, 21), (SECTIONS, FREQ, 3, D), jnp.float32), -4.0, 4.0)
    return (base * 0.2).astype(jnp.bfloat16)


def with_ends(result, rng, low, largest):
    place = [jax.random.randint(jax.random.fold_in(rng, axis), (), 0, length) for axis, length in enumerate(result.shape)]
    main_axis = result.shape.index(max(result.shape))
    next_to = place[:main_axis] + [(place[main_axis] + 1) % result.shape[main_axis]] + place[main_axis + 1:]
    return result.at[tuple(place)].set(low).at[tuple(next_to)].set(largest)


def level_of(key, extent, cuts, low, high):
    def one(position, blocks):
        heights = jax.random.uniform(jax.random.fold_in(jax.random.fold_in(key, 6), position), (blocks,), jnp.float32, low / len(cuts), high / len(cuts))
        return jnp.repeat(jnp.exp(heights), extent[position] // blocks).reshape((-1,) + (1,) * (len(extent) - position - 1))

    gain = one(*cuts[0])
    for cut in cuts[1:]:
        gain = gain * one(*cut)
    return gain


def scatter_about(own_key, extent, spread, limit, pieces=(), kind=jnp.bfloat16):
    result = jax.random.normal(own_key, extent, jnp.float32) * spread
    if len(pieces) > 0:
        result = level_of(own_key, extent, pieces, -0.22, 0.18) * result
    return jnp.clip(result, min=-limit, max=limit).astype(kind)


def setup_inputs(seed: int = 0) -> dict:
    seeds = jax.random.split(jax.random.key(seed), 7)
    return {
        "latents": scatter_about(seeds[0], (TOK, LATENTS, D), 1.0, 6.0, ((0, 16), (1, 8))),
        "timestep": with_ends(jax.random.randint(seeds[1], (LATENTS,), 0, 1000), jax.random.fold_in(seeds[1], 1), 0, 999).astype(jnp.int32),
        "target": draw_target(jax.random.fold_in(seeds[6], 71), 0),
        "qkv_weight": scatter_about(seeds[3], (SECTIONS, D, 3, D), D ** -0.5, 0.125, ((0, 8), (3, 16))),
        "mod_weight": draw_mod_weight(jax.random.fold_in(seeds[6], 71), 0),
        "out_weight": scatter_about(seeds[5], (SECTIONS, D, D), D ** -0.5, 0.125, ((0, 8), (1, 16))),
    }


def time_embed(steps):
    half_width = FREQ // 2
    frequency = jnp.exp(-math.log(10000.0) * jnp.arange(half_width, dtype=jnp.float32) / half_width)
    angles = steps.astype(jnp.float32)[:, None] * frequency[None, :]
    return jnp.concatenate([jnp.cos(angles), jnp.sin(angles)], axis=1)

def modulate(steps, mod_table):
    feature = jax.nn.silu(time_embed(steps))
    return jnp.einsum('bf,fcd->bcd', feature, mod_table.astype(jnp.float32), precision=lax.Precision.HIGHEST)

def normalize(values, shift, scale):
    row_mean = lax.optimization_barrier(jnp.mean(values, axis=-1, keepdims=True))
    centred = values - row_mean
    variance = lax.optimization_barrier(jnp.mean(centred * centred, axis=-1, keepdims=True))
    return centred * lax.rsqrt(variance + 1e-06) * (1.0 + scale) + shift

def reference(latents, timestep, target, qkv_weight, mod_weight, out_weight):

    def one_latent(index):
        tokens = lax.dynamic_index_in_dim(latents, index, 1, keepdims=False)
        section_id = lax.dynamic_index_in_dim(target, index, 0, keepdims=False)
        step_now = lax.dynamic_slice_in_dim(timestep, index, 1)
        table = lax.dynamic_index_in_dim(mod_weight, section_id, 0, keepdims=False)
        qkv_table = lax.dynamic_index_in_dim(qkv_weight, section_id, 0, keepdims=False)
        out_table = lax.dynamic_index_in_dim(out_weight, section_id, 0, keepdims=False)
        mods = modulate(step_now, table)[0]
        values = tokens.astype(jnp.float32)
        hidden = normalize(values, mods[0], mods[1]).astype(jnp.bfloat16)
        packed = jnp.dot(hidden, qkv_table.reshape(D, 3 * D), preferred_element_type=jnp.float32)
        packed = packed.astype(jnp.bfloat16).reshape(TOK, 3, HEADS, HEAD_DIM)
        query = packed[:, 0].astype(jnp.float32)
        keys = packed[:, 1].astype(jnp.float32)
        vals = packed[:, 2].astype(jnp.float32)
        scores = jnp.einsum('qhe,khe->hqk', query, keys) * HEAD_DIM ** (-0.5)
        soft = jax.nn.softmax(scores, axis=-1).astype(jnp.bfloat16)
        mixed = jnp.einsum('hqk,khe->qhe', soft.astype(jnp.float32), vals).astype(jnp.bfloat16)
        grouped = mixed.reshape(TOK, N_TP, D // N_TP).astype(jnp.float32)
        out_groups = out_table.reshape(N_TP, D // N_TP, D).astype(jnp.float32)
        partial_terms = jnp.einsum('sgk,gkd->gsd', grouped, out_groups).astype(jnp.bfloat16)
        partial_terms = lax.optimization_barrier(partial_terms)
        proj = lax.optimization_barrier(jnp.sum(partial_terms.astype(jnp.float32), axis=0))
        return (values + mods[2] * proj).astype(jnp.bfloat16)
    results = lax.map(one_latent, jnp.arange(LATENTS, dtype=jnp.int32))
    return jnp.moveaxis(results, 0, 1)
```

```python
import functools
import math

import jax
import jax.numpy as jnp
from jax import lax
from jax.experimental import pallas as pl
from jax.experimental.pallas import tpu as pltpu
from jax.sharding import PartitionSpec as P

HEAD_DIM = 128
FREQ = 256
MESH = pl.DeviceIdType.MESH
BF16 = jnp.bfloat16
F32 = jnp.float32


def time_embed(steps):
    half_width = FREQ // 2
    frequency = jnp.exp(-math.log(10000.0) * jnp.arange(half_width, dtype=F32) / half_width)
    angles = steps.astype(F32)[:, None] * frequency[None, :]
    return jnp.concatenate([jnp.cos(angles), jnp.sin(angles)], axis=1)


def split_feature(steps):
    feature = jax.nn.silu(time_embed(steps))
    high = lax.reduce_precision(feature, 8, 7)
    rest = feature - high
    mid = lax.reduce_precision(rest, 8, 7)
    low = rest - mid
    return jnp.concatenate([high, mid, low, jnp.zeros_like(low)], axis=0).astype(BF16)


def kernel(
    flag_ref, feat_ref, stay_ref, move_ref, mod_hbm, wqkv_hbm, wout_hbm,
    upd_ref,
    mod_v, mods, mod_send, mod_recv, hid_send,
    gath, w2, wo2, wn, wno, ws, wso,
    qkv, part, r3, r2, r1, r0,
    ld_sem, md_s, md_r, z_s, z_r, sw_s, sw_r, tok_s, tok_r, rs_s, rs_r,
):
    sections = lax.axis_size("section")
    tok = stay_ref.shape[0]
    sec = lax.axis_index("section")
    tp = lax.axis_index("tp")
    core = lax.rem(sec, 2)
    x = tp // 4
    y = lax.rem(tp, 4)
    u = jnp.where(core == 0, y, x)
    v = jnp.where(core == 0, x, y)

    def at(uu, vv):
        return jnp.where(core == 0, vv * 4 + uu, uu * 4 + vv)

    def flip(a):
        return a + 1 - 2 * lax.rem(a, 2)

    pair = (sec, at(flip(u), v))
    p1 = (sec, at(3 - u, v))
    p2 = (sec, at(u, flip(v)))
    p3 = (sec, at(u, 3 - v))
    before = (lax.rem(sec + sections - 1, sections), tp)
    after = (lax.rem(sec + 1, sections), tp)
    is_a = (u == 0) | (u == 3)
    moved = flag_ref[0] != 0

    def remote(src, dst, ssem, rsem, peer):
        return pltpu.make_async_remote_copy(
            src_ref=src, dst_ref=dst, send_sem=ssem, recv_sem=rsem,
            device_id=peer, device_id_type=MESH,
        )

    mod_load = pltpu.make_async_copy(mod_hbm, mod_v, ld_sem.at[0])
    mod_load.start()
    loads = [
        pltpu.make_async_copy(wqkv_hbm.at[i], w2.at[i, :, pl.ds(0, HEAD_DIM)], ld_sem.at[1 + i])
        for i in range(3)
    ]
    loads.append(pltpu.make_async_copy(wout_hbm, wo2.at[pl.ds(0, HEAD_DIM)], ld_sem.at[4]))
    for load in loads:
        load.start()

    barrier = pltpu.get_barrier_semaphore()
    for peer in (pair, p1, p2, p3, before, after):
        pl.semaphore_signal(barrier, inc=1, device_id=peer, device_id_type=MESH)
    pl.semaphore_wait(barrier, 6)

    z_copies = [
        remote(wqkv_hbm.at[i], wn.at[i], z_s.at[i], z_r.at[i], before) for i in range(3)
    ]
    z_copies.append(remote(wout_hbm, wno, z_s.at[3], z_r.at[3], before))

    mod_load.wait()
    mod_send[...] = jnp.zeros_like(mod_send)
    for c in range(3):
        prod = jnp.dot(feat_ref[...], mod_v[c], preferred_element_type=F32)
        full = prod[0:8] + prod[8:16] + prod[16:24]
        mods[c] = full
        mod_send[pl.ds(c, 1), :] = full[2:3]
    md = remote(mod_send, mod_recv, md_s, md_r, before)
    md.start()
    for copy in z_copies:
        copy.start()

    def norm(ref, shift, scale):
        values = ref[...].astype(F32)
        centred = values - jnp.mean(values, axis=-1, keepdims=True)
        variance = jnp.mean(centred * centred, axis=-1, keepdims=True)
        return (centred * lax.rsqrt(variance + 1e-06) * (1.0 + scale) + shift).astype(BF16)

    stay_hidden = norm(stay_ref, mods[0, 0:1, :], mods[1, 0:1, :])
    gath[0] = stay_hidden
    hid_send[...] = stay_hidden
    md.wait_recv()
    move_hidden = norm(
        move_ref,
        jnp.where(moved, mod_recv[0:1, :], mods[0, 1:2, :]),
        jnp.where(moved, mod_recv[1:2, :], mods[1, 1:2, :]),
    )
    gath[0] = jnp.where(is_a, gath[0], move_hidden)
    hid_send[...] = jnp.where(is_a, move_hidden, hid_send[...])

    t0 = remote(hid_send, gath.at[1], tok_s.at[0], tok_r.at[0], pair)
    d1 = [remote(gath.at[j], gath.at[2 + j], tok_s.at[1 + j], tok_r.at[1 + j], p1) for j in range(2)]
    d2 = [remote(gath.at[j], gath.at[4 + j], tok_s.at[3 + j], tok_r.at[3 + j], p2) for j in range(4)]
    d3 = [remote(gath.at[j], gath.at[8 + j], tok_s.at[7 + j], tok_r.at[7 + j], p3) for j in range(8)]
    t0.start()
    d1[0].start()
    d2[0].start()
    d3[0].start()

    swaps = [
        remote(ws.at[i], w2.at[i, :, pl.ds(HEAD_DIM, HEAD_DIM)], sw_s.at[i], sw_r.at[i], pair)
        for i in range(3)
    ]
    swaps.append(remote(wso, wo2.at[pl.ds(HEAD_DIM, HEAD_DIM)], sw_s.at[3], sw_r.at[3], pair))
    send_next = is_a & moved
    keep_next = jnp.logical_not(is_a) & moved

    def weight(i):
        loads[i].wait()
        z_copies[i].wait_recv()
        if i < 3:
            rows = w2.shape[1]
            step = min(512, rows)

            def piece(b, carry):
                rs = pl.ds(pl.multiple_of(b * step, step), step)
                own = w2[i, rs, pl.ds(0, HEAD_DIM)]
                nxt = wn[i, rs, :]
                ws[i, rs, :] = jnp.where(send_next, nxt, own)
                w2[i, rs, pl.ds(0, HEAD_DIM)] = jnp.where(keep_next, nxt, own)
                return carry

            lax.fori_loop(0, rows // step, piece, 0)
        else:
            own = wo2[pl.ds(0, HEAD_DIM), :]
            nxt = wno[...]
            wso[...] = jnp.where(send_next, nxt, own)
            wo2[pl.ds(0, HEAD_DIM), :] = jnp.where(keep_next, nxt, own)
        swaps[i].start()

    t0.wait_recv()
    d1[1].start()
    d2[1].start()
    d3[1].start()
    for j in range(2):
        d1[j].wait_recv()
        d2[2 + j].start()
        d3[2 + j].start()
    weight(0)
    for j in range(2):
        d2[j].wait_recv()
        d3[4 + j].start()
    weight(1)
    for j in range(2, 4):
        d2[j].wait_recv()
        d3[4 + j].start()
    weight(2)
    weight(3)
    for j in range(8):
        d3[j].wait_recv()

    slots = 4
    width = slots * tok
    depth = gath.shape[2]

    for i in range(3):
        swaps[i].wait_recv()

        def project(b, carry):
            rows = gath[pl.ds(b * slots, slots)].reshape(width, depth)
            out = jnp.dot(rows, w2[i], preferred_element_type=F32)
            qkv[i, pl.ds(pl.multiple_of(b * width, width), width), :] = out.astype(BF16)
            return carry

        lax.fori_loop(0, 16 // slots, project, 0)
    swaps[3].wait_recv()

    s3 = {j: remote(part.at[j], r3.at[j - 8], rs_s.at[j - 8], rs_r.at[j - 8], p3) for j in range(8, 16)}
    s2 = {j: remote(part.at[j], r2.at[j - 4], rs_s.at[4 + j], rs_r.at[4 + j], p2) for j in range(4, 8)}
    s1 = {j: remote(part.at[j], r1.at[j - 2], rs_s.at[10 + j], rs_r.at[10 + j], p1) for j in range(2, 4)}
    s0 = remote(part.at[1], r0, rs_s.at[14], rs_r.at[14], pair)

    factor = HEAD_DIM ** (-0.5) * math.log2(math.e)
    n_col = 4
    col = depth // n_col

    def attend(b):
        rows = pl.ds(b * width, width)
        heads = []
        for h in range(2):
            lanes = pl.ds(h * HEAD_DIM, HEAD_DIM)
            scores = lax.dot_general(
                qkv[0, rows, lanes], qkv[1, :, lanes], (((1,), (1,)), ((), ())),
                preferred_element_type=F32,
            )
            top = jnp.max(scores, axis=-1, keepdims=True)
            weights = jnp.exp2((scores - top) * factor)
            total = jnp.sum(weights, axis=-1, keepdims=True)
            mixed = jnp.dot(weights.astype(BF16), qkv[2, :, lanes], preferred_element_type=F32)
            heads.append((mixed / total).astype(BF16))
        both = jnp.concatenate(heads, axis=1)
        for n in range(n_col):
            lanes = pl.ds(n * col, col)
            out = jnp.dot(both, wo2[:, lanes], preferred_element_type=F32).astype(BF16)
            part[pl.ds(b * slots, slots), :, lanes] = out.reshape(slots, tok, col)

    for b in (3, 2, 1, 0):
        attend(b)
        if b >= 2:
            for j in reversed(range(b * slots, (b + 1) * slots)):
                s3[j].start()

    for j in (7, 6, 5, 4):
        s3[8 + j].wait_recv()
        part[j] = (part[j].astype(F32) + r3[j].astype(F32)).astype(BF16)
        s2[j].start()
    for j in (3, 2):
        s3[8 + j].wait_recv()
        s2[4 + j].wait_recv()
        part[j] = (part[j].astype(F32) + r3[j].astype(F32) + r2[j].astype(F32)).astype(BF16)
        s1[j].start()

    def total_of(j):
        s3[8 + j].wait_recv()
        s2[4 + j].wait_recv()
        s1[2 + j].wait_recv()
        return part[j].astype(F32) + r3[j].astype(F32) + r2[j].astype(F32) + r1[j].astype(F32)

    part[1] = total_of(1).astype(BF16)
    s0.start()
    keep = total_of(0)
    s0.wait_recv()
    other = r0[...].astype(F32)
    gate_move = jnp.where(moved, mod_recv[2:3, :], mods[2, 1:2, :])
    upd_ref[0] = (stay_ref[...].astype(F32) + mods[2, 0:1, :] * jnp.where(is_a, keep, other)).astype(BF16)
    upd_ref[1] = (move_ref[...].astype(F32) + gate_move * jnp.where(is_a, other, keep)).astype(BF16)

    md.wait_send()
    t0.wait_send()
    for copy in z_copies + swaps + d1 + d2 + d3:
        copy.wait_send()
    for copy in [*s3.values(), *s2.values(), *s1.values(), s0]:
        copy.wait_send()


def body(latents, timestep, target, qkv_weight, mod_weight, out_weight):
    slots = latents.shape[1]
    tok = latents.shape[0]
    depth = latents.shape[2]
    home = lax.axis_index("section")
    prev = jnp.maximum(home - 1, 0)
    own_target = lax.dynamic_slice_in_dim(target, home * slots, slots)
    prev_target = lax.dynamic_slice_in_dim(target, prev * slots, slots)
    own_steps = lax.dynamic_slice_in_dim(timestep, home * slots, slots)
    prev_steps = lax.dynamic_slice_in_dim(timestep, prev * slots, slots)
    first_moves = own_target[0] != home
    moved = first_moves | (own_target[1] != home)
    prev_first = prev_target[0] != prev
    stay_step = jnp.where(first_moves, own_steps[1], own_steps[0])
    move_step = jnp.where(first_moves, own_steps[0], own_steps[1])
    prev_step = jnp.where(prev_first, prev_steps[0], prev_steps[1])
    lane = jnp.arange(8, dtype=jnp.int32)
    steps = jnp.where(lane == 0, stay_step, jnp.where(lane == 1, move_step, prev_step))
    feature = split_feature(steps)
    stay = jnp.where(first_moves, latents[:, 1], latents[:, 0])
    move = jnp.where(first_moves, latents[:, 0], latents[:, 1])
    mod_table = jnp.transpose(mod_weight[0], (1, 0, 2))
    wqkv = jnp.transpose(qkv_weight[0], (1, 0, 2))
    wout = out_weight[0]
    vmem = pl.BlockSpec(memory_space=pltpu.VMEM)
    hbm = pl.BlockSpec(memory_space=pl.ANY)
    dma = pltpu.SemaphoreType.DMA
    updated = pl.pallas_call(
        kernel,
        out_shape=jax.ShapeDtypeStruct((2, tok, depth), BF16),
        in_specs=[pl.BlockSpec(memory_space=pltpu.SMEM), vmem, vmem, vmem, hbm, hbm, hbm],
        out_specs=vmem,
        scratch_shapes=[
            pltpu.VMEM(mod_table.shape, BF16),
            pltpu.VMEM((3, 8, depth), F32),
            pltpu.VMEM((8, depth), F32),
            pltpu.VMEM((8, depth), F32),
            pltpu.VMEM((tok, depth), BF16),
            pltpu.VMEM((16, tok, depth), BF16),
            pltpu.VMEM((3, depth, 2 * HEAD_DIM), BF16),
            pltpu.VMEM((2 * HEAD_DIM, depth), BF16),
            pltpu.VMEM((3, depth, HEAD_DIM), BF16),
            pltpu.VMEM((HEAD_DIM, depth), BF16),
            pltpu.VMEM((3, depth, HEAD_DIM), BF16),
            pltpu.VMEM((HEAD_DIM, depth), BF16),
            pltpu.VMEM((3, 16 * tok, 2 * HEAD_DIM), BF16),
            pltpu.VMEM((16, tok, depth), BF16),
            pltpu.VMEM((8, tok, depth), BF16),
            pltpu.VMEM((4, tok, depth), BF16),
            pltpu.VMEM((2, tok, depth), BF16),
            pltpu.VMEM((tok, depth), BF16),
            dma((5,)),
            dma,
            dma,
            dma((4,)),
            dma((4,)),
            dma((4,)),
            dma((4,)),
            dma((15,)),
            dma((15,)),
            dma((15,)),
            dma((15,)),
        ],
        compiler_params=pltpu.CompilerParams(
            collective_id=0, has_side_effects=True, vmem_limit_bytes=56 * 1024 * 1024
        ),
    )(moved.astype(jnp.int32)[None], feature, stay, move, mod_table, wqkv, wout)
    first = jnp.where(first_moves, updated[1], updated[0])
    second = jnp.where(first_moves, updated[0], updated[1])
    return jnp.stack([first, second], axis=1)


def solution(mesh):
    return jax.shard_map(
        body,
        mesh=mesh,
        in_specs=(
            P("tp", "section", None),
            P(),
            P(),
            P("section", None, None, "tp"),
            P("section", None, None, None),
            P("section", "tp", None),
        ),
        out_specs=P("tp", "section", None),
        check_vma=False,
    )
```

```python
import functools
import math

import jax
import jax.numpy as jnp
from jax import lax
from jax.experimental import pallas as pl
from jax.experimental.pallas import tpu as pltpu
from jax.sharding import PartitionSpec as P

HEAD_DIM = 128
FREQ = 256
MESH = pl.DeviceIdType.MESH
BF16 = jnp.bfloat16
F32 = jnp.float32


def time_embed(steps):
    half_width = FREQ // 2
    frequency = jnp.exp(-math.log(10000.0) * jnp.arange(half_width, dtype=F32) / half_width)
    angles = steps.astype(F32)[:, None] * frequency[None, :]
    return jnp.concatenate([jnp.cos(angles), jnp.sin(angles)], axis=1)


def split_feature(steps):
    feature = jax.nn.silu(time_embed(steps))
    high = lax.reduce_precision(feature, 8, 7)
    rest = feature - high
    mid = lax.reduce_precision(rest, 8, 7)
    low = rest - mid
    return jnp.concatenate([high, mid, low], axis=0).astype(BF16)


def kernel(
    target_ref, feat_ref, lat_ref, mod_hbm, wqkv_hbm, wout_hbm,
    upd_ref,
    mod_v, mods, mod_send, mod_recv, hid_send,
    gath, w2, wo2, wn, wno, ws, wso,
    qkv, part, r3, r2, r1, r0,
    ld_sem, md_s, md_r, z_s, z_r, sw_s, sw_r, tok_s, tok_r, rs_s, rs_r,
):
    sections = lax.axis_size("section")
    tok = lat_ref.shape[1]
    latents = feat_ref.shape[0] // 3
    sec = lax.axis_index("section")
    tp = lax.axis_index("tp")
    core = lax.rem(sec, 2)
    x = tp // 4
    y = lax.rem(tp, 4)
    u = jnp.where(core == 0, y, x)
    v = jnp.where(core == 0, x, y)

    def at(uu, vv):
        return jnp.where(core == 0, vv * 4 + uu, uu * 4 + vv)

    def flip(a):
        return a + 1 - 2 * lax.rem(a, 2)

    pair = (sec, at(flip(u), v))
    p1 = (sec, at(3 - u, v))
    p2 = (sec, at(u, flip(v)))
    p3 = (sec, at(u, 3 - v))
    before = (lax.rem(sec + sections - 1, sections), tp)
    after = (lax.rem(sec + 1, sections), tp)
    is_a = (u == 0) | (u == 3)
    prev = jnp.maximum(sec - 1, 0)
    first_moves = target_ref[2 * sec] != sec
    moved = first_moves | (target_ref[2 * sec + 1] != sec)
    prev_first = target_ref[2 * prev] != prev

    def remote(src, dst, ssem, rsem, peer):
        return pltpu.make_async_remote_copy(
            src_ref=src, dst_ref=dst, send_sem=ssem, recv_sem=rsem,
            device_id=peer, device_id_type=MESH,
        )

    mod_load = pltpu.make_async_copy(mod_hbm, mod_v, ld_sem.at[0])
    mod_load.start()
    loads = [
        pltpu.make_async_copy(wqkv_hbm.at[i], w2.at[i, :, pl.ds(0, HEAD_DIM)], ld_sem.at[1 + i])
        for i in range(3)
    ]
    loads.append(pltpu.make_async_copy(wout_hbm, wo2.at[pl.ds(0, HEAD_DIM)], ld_sem.at[4]))
    for load in loads:
        load.start()

    barrier = pltpu.get_barrier_semaphore()
    for peer in (pair, p1, p2, p3, before, after):
        pl.semaphore_signal(barrier, inc=1, device_id=peer, device_id_type=MESH)
    pl.semaphore_wait(barrier, 6)

    z_copies = [
        remote(wqkv_hbm.at[i], wn.at[i], z_s.at[i], z_r.at[i], before) for i in range(3)
    ]
    z_copies.append(remote(wout_hbm, wno, z_s.at[3], z_r.at[3], before))

    mod_load.wait()
    mod_send[...] = jnp.zeros_like(mod_send)
    for c in range(3):
        prod = jnp.dot(feat_ref[...], mod_v[c], preferred_element_type=F32)
        mods[c] = prod[0:latents] + prod[latents : 2 * latents] + prod[2 * latents : 3 * latents]
        mod_send[pl.ds(c, 1), :] = jnp.where(
            prev_first, mods[c, pl.ds(2 * prev, 1), :], mods[c, pl.ds(2 * prev + 1, 1), :]
        )
    md = remote(mod_send, mod_recv, md_s, md_r, before)
    md.start()
    for copy in z_copies:
        copy.start()

    def mod_row(c, moving):
        first = mods[c, pl.ds(2 * sec, 1), :]
        second = mods[c, pl.ds(2 * sec + 1, 1), :]
        if moving:
            return jnp.where(moved, mod_recv[pl.ds(c, 1), :], jnp.where(first_moves, first, second))
        return jnp.where(first_moves, second, first)

    def tokens(moving):
        if moving:
            return jnp.where(first_moves, lat_ref[0], lat_ref[1]).astype(F32)
        return jnp.where(first_moves, lat_ref[1], lat_ref[0]).astype(F32)

    def norm(moving):
        values = tokens(moving)
        shift, scale = mod_row(0, moving), mod_row(1, moving)
        centred = values - jnp.mean(values, axis=-1, keepdims=True)
        variance = jnp.mean(centred * centred, axis=-1, keepdims=True)
        return (centred * lax.rsqrt(variance + 1e-06) * (1.0 + scale) + shift).astype(BF16)

    stay_hidden = norm(False)
    gath[0] = stay_hidden
    hid_send[...] = stay_hidden
    md.wait_recv()
    move_hidden = norm(True)
    gath[0] = jnp.where(is_a, gath[0], move_hidden)
    hid_send[...] = jnp.where(is_a, move_hidden, hid_send[...])

    t0 = remote(hid_send, gath.at[1], tok_s.at[0], tok_r.at[0], pair)
    d1 = [remote(gath.at[j], gath.at[2 + j], tok_s.at[1 + j], tok_r.at[1 + j], p1) for j in range(2)]
    d2 = [remote(gath.at[j], gath.at[4 + j], tok_s.at[3 + j], tok_r.at[3 + j], p2) for j in range(4)]
    d3 = [remote(gath.at[j], gath.at[8 + j], tok_s.at[7 + j], tok_r.at[7 + j], p3) for j in range(8)]
    t0.start()
    d1[0].start()
    d2[0].start()
    d3[0].start()

    swaps = [
        remote(ws.at[i], w2.at[i, :, pl.ds(HEAD_DIM, HEAD_DIM)], sw_s.at[i], sw_r.at[i], pair)
        for i in range(3)
    ]
    swaps.append(remote(wso, wo2.at[pl.ds(HEAD_DIM, HEAD_DIM)], sw_s.at[3], sw_r.at[3], pair))
    send_next = is_a & moved
    keep_next = jnp.logical_not(is_a) & moved

    def weight(i):
        loads[i].wait()
        z_copies[i].wait_recv()
        if i < 3:
            rows = w2.shape[1]
            step = min(512, rows)

            def piece(b, carry):
                rs = pl.ds(pl.multiple_of(b * step, step), step)
                own = w2[i, rs, pl.ds(0, HEAD_DIM)]
                nxt = wn[i, rs, :]
                ws[i, rs, :] = jnp.where(send_next, nxt, own)
                w2[i, rs, pl.ds(0, HEAD_DIM)] = jnp.where(keep_next, nxt, own)
                return carry

            lax.fori_loop(0, rows // step, piece, 0)
        else:
            own = wo2[pl.ds(0, HEAD_DIM), :]
            nxt = wno[...]
            wso[...] = jnp.where(send_next, nxt, own)
            wo2[pl.ds(0, HEAD_DIM), :] = jnp.where(keep_next, nxt, own)
        swaps[i].start()

    t0.wait_recv()
    d1[1].start()
    d2[1].start()
    d3[1].start()
    for j in range(2):
        d1[j].wait_recv()
        d2[2 + j].start()
        d3[2 + j].start()
    weight(0)
    for j in range(2):
        d2[j].wait_recv()
        d3[4 + j].start()
    weight(1)
    for j in range(2, 4):
        d2[j].wait_recv()
        d3[4 + j].start()
    weight(2)
    weight(3)
    for j in range(8):
        d3[j].wait_recv()

    slots = 4
    width = slots * tok
    depth = gath.shape[2]

    for i in range(3):
        swaps[i].wait_recv()

        def project(b, carry):
            rows = gath[pl.ds(b * slots, slots)].reshape(width, depth)
            out = jnp.dot(rows, w2[i], preferred_element_type=F32)
            qkv[i, pl.ds(pl.multiple_of(b * width, width), width), :] = out.astype(BF16)
            return carry

        lax.fori_loop(0, 16 // slots, project, 0)
    swaps[3].wait_recv()

    s3 = {j: remote(part.at[j], r3.at[j - 8], rs_s.at[j - 8], rs_r.at[j - 8], p3) for j in range(8, 16)}
    s2 = {j: remote(part.at[j], r2.at[j - 4], rs_s.at[4 + j], rs_r.at[4 + j], p2) for j in range(4, 8)}
    s1 = {j: remote(part.at[j], r1.at[j - 2], rs_s.at[10 + j], rs_r.at[10 + j], p1) for j in range(2, 4)}
    s0 = remote(part.at[1], r0, rs_s.at[14], rs_r.at[14], pair)

    factor = HEAD_DIM ** (-0.5) * math.log2(math.e)
    n_col = 4
    col = depth // n_col

    def attend(b):
        rows = pl.ds(b * width, width)
        heads = []
        for h in range(2):
            lanes = pl.ds(h * HEAD_DIM, HEAD_DIM)
            scores = lax.dot_general(
                qkv[0, rows, lanes], qkv[1, :, lanes], (((1,), (1,)), ((), ())),
                preferred_element_type=F32,
            )
            top = jnp.max(scores, axis=-1, keepdims=True)
            weights = jnp.exp2((scores - top) * factor)
            total = jnp.sum(weights, axis=-1, keepdims=True)
            mixed = jnp.dot(weights.astype(BF16), qkv[2, :, lanes], preferred_element_type=F32)
            heads.append((mixed / total).astype(BF16))
        both = jnp.concatenate(heads, axis=1)
        for n in range(n_col):
            lanes = pl.ds(n * col, col)
            out = jnp.dot(both, wo2[:, lanes], preferred_element_type=F32).astype(BF16)
            part[pl.ds(b * slots, slots), :, lanes] = out.reshape(slots, tok, col)

    for b in (3, 2, 1, 0):
        attend(b)
        if b >= 2:
            for j in reversed(range(b * slots, (b + 1) * slots)):
                s3[j].start()

    for j in (7, 6, 5, 4):
        s3[8 + j].wait_recv()
        part[j] = (part[j].astype(F32) + r3[j].astype(F32)).astype(BF16)
        s2[j].start()
    for j in (3, 2):
        s3[8 + j].wait_recv()
        s2[4 + j].wait_recv()
        part[j] = (part[j].astype(F32) + r3[j].astype(F32) + r2[j].astype(F32)).astype(BF16)
        s1[j].start()

    def total_of(j):
        s3[8 + j].wait_recv()
        s2[4 + j].wait_recv()
        s1[2 + j].wait_recv()
        return part[j].astype(F32) + r3[j].astype(F32) + r2[j].astype(F32) + r1[j].astype(F32)

    part[1] = total_of(1).astype(BF16)
    s0.start()
    keep = total_of(0)
    s0.wait_recv()
    other = r0[...].astype(F32)
    stay_out = (tokens(False) + mod_row(2, False) * jnp.where(is_a, keep, other)).astype(BF16)
    move_out = (tokens(True) + mod_row(2, True) * jnp.where(is_a, other, keep)).astype(BF16)
    upd_ref[0] = jnp.where(first_moves, move_out, stay_out)
    upd_ref[1] = jnp.where(first_moves, stay_out, move_out)

    md.wait_send()
    t0.wait_send()
    for copy in z_copies + swaps + d1 + d2 + d3:
        copy.wait_send()
    for copy in [*s3.values(), *s2.values(), *s1.values(), s0]:
        copy.wait_send()


def body(latents, timestep, target, qkv_weight, mod_weight, out_weight):
    tok = latents.shape[0]
    depth = latents.shape[2]
    feature = split_feature(timestep)
    mod_table = jnp.transpose(mod_weight[0], (1, 0, 2))
    wqkv = jnp.transpose(qkv_weight[0], (1, 0, 2))
    wout = out_weight[0]
    vmem = pl.BlockSpec(memory_space=pltpu.VMEM)
    hbm = pl.BlockSpec(memory_space=pl.ANY)
    dma = pltpu.SemaphoreType.DMA
    updated = pl.pallas_call(
        kernel,
        out_shape=jax.ShapeDtypeStruct((2, tok, depth), BF16),
        in_specs=[pl.BlockSpec(memory_space=pltpu.SMEM), vmem, vmem, hbm, hbm, hbm],
        out_specs=vmem,
        scratch_shapes=[
            pltpu.VMEM(mod_table.shape, BF16),
            pltpu.VMEM((3, timestep.shape[0], depth), F32),
            pltpu.VMEM((8, depth), F32),
            pltpu.VMEM((8, depth), F32),
            pltpu.VMEM((tok, depth), BF16),
            pltpu.VMEM((16, tok, depth), BF16),
            pltpu.VMEM((3, depth, 2 * HEAD_DIM), BF16),
            pltpu.VMEM((2 * HEAD_DIM, depth), BF16),
            pltpu.VMEM((3, depth, HEAD_DIM), BF16),
            pltpu.VMEM((HEAD_DIM, depth), BF16),
            pltpu.VMEM((3, depth, HEAD_DIM), BF16),
            pltpu.VMEM((HEAD_DIM, depth), BF16),
            pltpu.VMEM((3, 16 * tok, 2 * HEAD_DIM), BF16),
            pltpu.VMEM((16, tok, depth), BF16),
            pltpu.VMEM((8, tok, depth), BF16),
            pltpu.VMEM((4, tok, depth), BF16),
            pltpu.VMEM((2, tok, depth), BF16),
            pltpu.VMEM((tok, depth), BF16),
            dma((5,)),
            dma,
            dma,
            dma((4,)),
            dma((4,)),
            dma((4,)),
            dma((4,)),
            dma((15,)),
            dma((15,)),
            dma((15,)),
            dma((15,)),
        ],
        compiler_params=pltpu.CompilerParams(
            collective_id=0, has_side_effects=True, vmem_limit_bytes=56 * 1024 * 1024
        ),
    )(target, feature, jnp.transpose(latents, (1, 0, 2)), mod_table, wqkv, wout)
    return jnp.transpose(updated, (1, 0, 2))


def solution(mesh):
    return jax.shard_map(
        body,
        mesh=mesh,
        in_specs=(
            P("tp", "section", None),
            P(),
            P(),
            P("section", None, None, "tp"),
            P("section", None, None, None),
            P("section", "tp", None),
        ),
        out_specs=P("tp", "section", None),
        check_vma=False,
    )
```

```python
import functools
import math

import jax
import jax.numpy as jnp
from jax import lax
from jax.experimental import pallas as pl
from jax.experimental.pallas import tpu as pltpu
from jax.sharding import PartitionSpec as P

HEAD_DIM = 128
FREQ = 256
MESH = pl.DeviceIdType.MESH
BF16 = jnp.bfloat16
F32 = jnp.float32


def time_embed(steps):
    half_width = FREQ // 2
    frequency = jnp.exp(-math.log(10000.0) * jnp.arange(half_width, dtype=F32) / half_width)
    angles = steps.astype(F32)[:, None] * frequency[None, :]
    return jnp.concatenate([jnp.cos(angles), jnp.sin(angles)], axis=1)


def split_feature(steps):
    feature = jax.nn.silu(time_embed(steps))
    high = lax.reduce_precision(feature, 8, 7)
    rest = feature - high
    mid = lax.reduce_precision(rest, 8, 7)
    low = rest - mid
    return jnp.concatenate([high, mid, low], axis=0).astype(BF16)


def kernel(
    target_ref, feat_ref, lat_ref, mod_hbm, wqkv_hbm, wout_hbm,
    upd_ref,
    mod_v, mods, mod_send, mod_recv, hid_send,
    gath, w2, wo2, wn, wno, ws, wso,
    qkv, part, rf, rg, r1, r0,
    ld_sem, md_s, md_r, z_s, z_r, sw_s, sw_r, tok_s, tok_r, rs_s, rs_r,
):
    sections = lax.axis_size("section")
    tok = lat_ref.shape[1]
    depth = lat_ref.shape[2]
    latents = feat_ref.shape[0] // 3
    sec = lax.axis_index("section")
    tp = lax.axis_index("tp")
    core = lax.rem(sec, 2)
    x = tp // 4
    y = lax.rem(tp, 4)
    u = jnp.where(core == 0, y, x)
    v = jnp.where(core == 0, x, y)

    def at(uu, vv):
        return jnp.where(core == 0, vv * 4 + uu, uu * 4 + vv)

    def flip(a):
        return a + 1 - 2 * lax.rem(a, 2)

    pair = (sec, at(flip(u), v))
    p1 = (sec, at(3 - u, v))
    p2 = (sec, at(u, flip(v)))
    p3 = (sec, at(u, 3 - v))
    before = (lax.rem(sec + sections - 1, sections), tp)
    after = (lax.rem(sec + 1, sections), tp)
    is_a = (u == 0) | (u == 3)
    is_b = jnp.logical_not(is_a)
    prev = jnp.maximum(sec - 1, 0)
    first_moves = target_ref[2 * sec] != sec
    moved = first_moves | (target_ref[2 * sec + 1] != sec)
    prev_first = target_ref[2 * prev] != prev

    def remote(src, dst, ssem, rsem, peer):
        return pltpu.make_async_remote_copy(
            src_ref=src, dst_ref=dst, send_sem=ssem, recv_sem=rsem,
            device_id=peer, device_id_type=MESH,
        )

    own_lanes = pl.ds(0, HEAD_DIM)
    pair_lanes = pl.ds(HEAD_DIM, HEAD_DIM)
    mod_loads = [pltpu.make_async_copy(mod_hbm.at[c], mod_v.at[c], ld_sem.at[4 + c]) for c in range(3)]
    for load in mod_loads:
        load.start()

    barrier = pltpu.get_barrier_semaphore()
    for peer in (pair, p1, p2, p3, before, after):
        pl.semaphore_signal(barrier, inc=1, device_id=peer, device_id_type=MESH)
    pl.semaphore_wait(barrier, 6)

    z_copies = [
        remote(wqkv_hbm.at[i], wn.at[i], z_s.at[i], z_r.at[i], before) for i in range(1, 3)
    ]
    z_copies.append(remote(wout_hbm, wno, z_s.at[3], z_r.at[3], before))
    rows_half = wn.shape[1] // 2
    z_first = [
        remote(wqkv_hbm.at[0, rs], wn.at[0, rs], z_s.at[4 * k], z_r.at[4 * k], before)
        for k, rs in enumerate((pl.ds(0, rows_half), pl.ds(rows_half, rows_half)))
    ]

    def next_arrived(i):
        for copy in z_first if i == 0 else z_copies[i - 1 : i]:
            copy.wait_recv()

    direct = [
        remote(wqkv_hbm.at[i], w2.at[i, :, pair_lanes], sw_s.at[i], sw_r.at[i], pair)
        for i in range(3)
    ]
    direct.append(remote(wout_hbm, wo2.at[pair_lanes], sw_s.at[3], sw_r.at[3], pair))
    chosen = [
        remote(ws.at[i], w2.at[i, :, pair_lanes], sw_s.at[i], sw_r.at[i], pair)
        for i in range(3)
    ]
    chosen.append(remote(wso, wo2.at[pair_lanes], sw_s.at[3], sw_r.at[3], pair))
    z_first[0].start()

    @pl.when(is_b)
    def _():
        direct[0].start()

    loads = [
        pltpu.make_async_copy(wqkv_hbm.at[i], w2.at[i, :, own_lanes], ld_sem.at[i])
        for i in range(3)
    ]
    loads.append(pltpu.make_async_copy(wout_hbm, wo2.at[own_lanes], ld_sem.at[3]))
    loads[0].start()

    def select_weight(i, take_next, in_place):
        if i < 3:
            rows = w2.shape[1]
            step = min(512, rows)

            def piece(b, carry):
                rs = pl.ds(pl.multiple_of(b * step, step), step)
                picked = jnp.where(take_next, wn[i, rs, :], w2[i, rs, own_lanes])
                if in_place:
                    w2[i, rs, own_lanes] = picked
                else:
                    ws[i, rs, :] = picked
                return carry

            lax.fori_loop(0, rows // step, piece, 0)
        else:
            picked = jnp.where(take_next, wno[...], wo2[own_lanes, :])
            if in_place:
                wo2[own_lanes, :] = picked
            else:
                wso[...] = picked

    def send_weight(i, which):
        @pl.when(is_a & (core == which))
        def _():
            loads[i].wait()
            next_arrived(i)
            select_weight(i, moved, False)
            chosen[i].start()

    def make_mods(c):
        mod_loads[c].wait()
        prod = jnp.dot(feat_ref[...], mod_v[c], preferred_element_type=F32)
        mods[c] = prod[0:latents] + prod[latents : 2 * latents] + prod[2 * latents : 3 * latents]
        mod_send[c // 2, pl.ds(c % 2, 1), :] = jnp.where(
            prev_first, mods[c, pl.ds(2 * prev, 1), :], mods[c, pl.ds(2 * prev + 1, 1), :]
        )

    mod_send[...] = jnp.zeros_like(mod_send)
    md = [remote(mod_send.at[k], mod_recv.at[k], md_s.at[k], md_r.at[k], before) for k in range(2)]
    make_mods(0)
    make_mods(1)
    md[0].start()
    z_first[1].start()
    for copy in z_copies:
        copy.start()
    for load in loads[1:]:
        load.start()

    def mod_row(c, moving):
        first = mods[c, pl.ds(2 * sec, 1), :]
        second = mods[c, pl.ds(2 * sec + 1, 1), :]
        if moving:
            arrived = mod_recv[c // 2, pl.ds(c % 2, 1), :]
            return jnp.where(moved, arrived, jnp.where(first_moves, first, second))
        return jnp.where(first_moves, second, first)

    def tokens(moving):
        if moving:
            return jnp.where(first_moves, lat_ref[0], lat_ref[1]).astype(F32)
        return jnp.where(first_moves, lat_ref[1], lat_ref[0]).astype(F32)

    def centre(moving):
        values = tokens(moving)
        centred = values - jnp.mean(values, axis=-1, keepdims=True)
        variance = jnp.mean(centred * centred, axis=-1, keepdims=True)
        return centred * lax.rsqrt(variance + 1e-06)

    def modulate(normed, moving):
        return (normed * (1.0 + mod_row(1, moving)) + mod_row(0, moving)).astype(BF16)

    cuts = 2
    piece_rows = tok // cuts

    def place(p):
        return gath.at[p // cuts, pl.ds((p % cuts) * piece_rows, piece_rows)]

    def doubling(slots_before, peer):
        count, first_sem = slots_before * cuts, (slots_before - 1) * cuts
        return [
            remote(place(p), place(count + p), tok_s.at[first_sem + p], tok_r.at[first_sem + p], peer)
            for p in range(count)
        ]

    t0 = [
        remote(hid_send.at[pl.ds(p * piece_rows, piece_rows)], place(cuts + p), tok_s.at[p], tok_r.at[p], pair)
        for p in range(cuts)
    ]
    d1, d2, d3 = doubling(2, p1), doubling(4, p2), doubling(8, p3)

    def pass_on(p):
        d3[p].start()
        if p < 4 * cuts:
            d2[p].start()
        if p < 2 * cuts:
            d1[p].start()

    stay_hidden = modulate(centre(False), False)

    @pl.when(is_a)
    def _():
        gath[0] = stay_hidden
        for p in range(cuts):
            pass_on(p)

    @pl.when(is_b)
    def _():
        hid_send[...] = stay_hidden
        for copy in t0:
            copy.start()

    send_weight(0, 0)
    md[0].wait_recv()
    move_hidden = modulate(centre(True), True)

    @pl.when(is_a)
    def _():
        hid_send[...] = move_hidden
        for copy in t0:
            copy.start()

    @pl.when(is_b)
    def _():
        gath[0] = move_hidden
        for p in range(cuts):
            pass_on(p)
        for i in range(1, 4):
            direct[i].start()

    make_mods(2)
    md[1].start()
    send_weight(1, 0)
    send_weight(0, 1)
    for p in range(cuts):
        t0[p].wait_recv()
        pass_on(cuts + p)
    send_weight(2, 0)
    for p in range(2 * cuts):
        d1[p].wait_recv()
        pass_on(2 * cuts + p)
    send_weight(3, 0)
    send_weight(1, 1)
    for p in range(2 * cuts):
        d2[p].wait_recv()
        pass_on(4 * cuts + p)
    send_weight(2, 1)
    for p in range(2 * cuts, 4 * cuts):
        d2[p].wait_recv()
        pass_on(4 * cuts + p)
    send_weight(3, 1)

    slots = 4
    width = slots * tok

    @pl.when(is_b)
    def _():
        for i in range(4):
            loads[i].wait()
            next_arrived(i)
            select_weight(i, moved, True)

    def project(i, b):
        rows = gath[pl.ds(b * slots, slots)].reshape(width, depth)
        out = jnp.dot(rows, w2[i], preferred_element_type=F32)
        qkv[i, pl.ds(b * width, width), :] = out.astype(BF16)

    for i in range(3):
        chosen[i].wait_recv()
        project(i, 0)
        project(i, 1)
    for b in (2, 3):
        for p in range(4 * cuts):
            d3[4 * cuts * (b - 2) + p].wait_recv()
        for i in range(3):
            project(i, b)
    chosen[3].wait_recv()

    half = depth // 2
    lanes_of = [pl.ds(0, half), pl.ds(half, half)]

    def low(j):
        return j if j < 4 else j - 4

    first, second, third, fourth = [{}, {}], [{}, {}], [{}, {}], []
    for h in range(2):
        lanes = lanes_of[h]
        jump = 8 - 4 * h
        goals = range(8) if h == 0 else (0, 1, 2, 3, 8, 9, 10, 11)

        def hop(src, dst, sem, peer):
            return remote(src, dst, rs_s.at[15 * h + sem], rs_r.at[15 * h + sem], peer)

        for n, j in enumerate(goals):
            first[h][j] = hop(part.at[j + jump, :, lanes], rf.at[h, n], n, (p3, p2)[h])
        for j in range(4):
            second[h][j] = hop(part.at[j + 12 - jump, :, lanes], rg.at[h, j], 8 + j, (p2, p3)[h])
        for j in range(2):
            third[h][j] = hop(part.at[j + 2, :, lanes], r1.at[j, :, lanes], 12 + j, p1)
        fourth.append(hop(part.at[1, :, lanes], r0.at[:, lanes], 14, pair))

    factor = HEAD_DIM ** (-0.5) * math.log2(math.e)
    n_col = 4
    col = depth // n_col

    def attend(b):
        rows = pl.ds(b * width, width)
        heads = []
        for h in range(2):
            lanes = pl.ds(h * HEAD_DIM, HEAD_DIM)
            scores = lax.dot_general(
                qkv[0, rows, lanes], qkv[1, :, lanes], (((1,), (1,)), ((), ())),
                preferred_element_type=F32,
            )
            top = jnp.max(scores, axis=-1, keepdims=True)
            weights = jnp.exp2((scores - top) * factor)
            total = jnp.sum(weights, axis=-1, keepdims=True)
            mixed = jnp.dot(weights.astype(BF16), qkv[2, :, lanes], preferred_element_type=F32)
            heads.append((mixed / total).astype(BF16))
        both = jnp.concatenate(heads, axis=1)
        for n in range(n_col):
            lanes = pl.ds(n * col, col)
            out = jnp.dot(both, wo2[:, lanes], preferred_element_type=F32).astype(BF16)
            part[pl.ds(b * slots, slots), :, lanes] = out.reshape(slots, tok, col)

    def begin(*goals):
        for h, j in goals:
            first[h][j].start()

    def second_stage(k):
        for h in range(2):
            j = k + 4 + 4 * h
            first[h][j].wait_recv()
            arrived = rf[h, j - 4 * h].astype(F32)
            part[j, :, lanes_of[h]] = (part[j, :, lanes_of[h]].astype(F32) + arrived).astype(BF16)
            second[h][k].start()

    def settle(k, h):
        first[h][k].wait_recv()
        second[h][k].wait_recv()
        own = part[k, :, lanes_of[h]].astype(F32)
        return own + rf[h, k].astype(F32) + rg[h, k].astype(F32)

    def third_stage(k):
        for h in range(2):
            part[k, :, lanes_of[h]] = settle(k, h).astype(BF16)
            third[h][k - 2].start()

    def finish(k, h):
        total = settle(k, h)
        third[h][k].wait_recv()
        return total + r1[k, :, lanes_of[h]].astype(F32)

    attend(3)
    begin((0, 7), (1, 11), (0, 5), (1, 9))
    attend(2)
    begin((0, 3), (0, 1))
    attend(1)
    begin((1, 3), (1, 1))
    attend(0)
    second_stage(3)
    second_stage(1)
    begin((0, 6), (1, 10), (0, 2), (1, 2), (0, 4), (1, 8), (0, 0), (1, 0))
    third_stage(3)
    second_stage(2)
    second_stage(0)
    for h in range(2):
        part[1, :, lanes_of[h]] = finish(1, h).astype(BF16)
        fourth[h].start()
    third_stage(2)
    keep = jnp.concatenate([finish(0, 0), finish(0, 1)], axis=1)
    md[1].wait_recv()
    for copy in fourth:
        copy.wait_recv()
    other = r0[...].astype(F32)
    stay_out = (tokens(False) + mod_row(2, False) * jnp.where(is_a, keep, other)).astype(BF16)
    move_out = (tokens(True) + mod_row(2, True) * jnp.where(is_a, other, keep)).astype(BF16)
    upd_ref[0] = jnp.where(first_moves, move_out, stay_out)
    upd_ref[1] = jnp.where(first_moves, stay_out, move_out)

    for copy in [*md, *z_first, *z_copies, *chosen, *t0, *d1, *d2, *d3, *fourth]:
        copy.wait_send()
    for group in (*first, *second, *third):
        for copy in group.values():
            copy.wait_send()


def body(latents, timestep, target, qkv_weight, mod_weight, out_weight):
    tok = latents.shape[0]
    depth = latents.shape[2]
    feature = split_feature(timestep)
    mod_table = jnp.transpose(mod_weight[0], (1, 0, 2))
    wqkv = jnp.transpose(qkv_weight[0], (1, 0, 2))
    wout = out_weight[0]
    vmem = pl.BlockSpec(memory_space=pltpu.VMEM)
    hbm = pl.BlockSpec(memory_space=pl.ANY)
    dma = pltpu.SemaphoreType.DMA
    updated = pl.pallas_call(
        kernel,
        out_shape=jax.ShapeDtypeStruct((2, tok, depth), BF16),
        in_specs=[pl.BlockSpec(memory_space=pltpu.SMEM), vmem, vmem, hbm, hbm, hbm],
        out_specs=vmem,
        scratch_shapes=[
            pltpu.VMEM(mod_table.shape, BF16),
            pltpu.VMEM((3, timestep.shape[0], depth), F32),
            pltpu.VMEM((2, 8, depth), F32),
            pltpu.VMEM((2, 8, depth), F32),
            pltpu.VMEM((tok, depth), BF16),
            pltpu.VMEM((16, tok, depth), BF16),
            pltpu.VMEM((3, depth, 2 * HEAD_DIM), BF16),
            pltpu.VMEM((2 * HEAD_DIM, depth), BF16),
            pltpu.VMEM((3, depth, HEAD_DIM), BF16),
            pltpu.VMEM((HEAD_DIM, depth), BF16),
            pltpu.VMEM((3, depth, HEAD_DIM), BF16),
            pltpu.VMEM((HEAD_DIM, depth), BF16),
            pltpu.VMEM((3, 16 * tok, 2 * HEAD_DIM), BF16),
            pltpu.VMEM((16, tok, depth), BF16),
            pltpu.VMEM((2, 8, tok, depth // 2), BF16),
            pltpu.VMEM((2, 4, tok, depth // 2), BF16),
            pltpu.VMEM((2, tok, depth), BF16),
            pltpu.VMEM((tok, depth), BF16),
            dma((7,)),
            dma((2,)),
            dma((2,)),
            dma((5,)),
            dma((5,)),
            dma((4,)),
            dma((4,)),
            dma((30,)),
            dma((30,)),
            dma((30,)),
            dma((30,)),
        ],
        compiler_params=pltpu.CompilerParams(
            collective_id=0, has_side_effects=True, vmem_limit_bytes=54 * 1024 * 1024
        ),
    )(target, feature, jnp.transpose(latents, (1, 0, 2)), mod_table, wqkv, wout)
    return jnp.transpose(updated, (1, 0, 2))


def solution(mesh):
    return jax.shard_map(
        body,
        mesh=mesh,
        in_specs=(
            P("tp", "section", None),
            P(),
            P(),
            P("section", None, None, "tp"),
            P("section", None, None, None),
            P("section", "tp", None),
        ),
        out_specs=P("tp", "section", None),
        check_vma=False,
    )
```

```python
import functools
import math

import jax
import jax.numpy as jnp
from jax import lax
from jax.experimental import pallas as pl
from jax.experimental.pallas import tpu as pltpu
from jax.sharding import PartitionSpec as P

HEAD_DIM = 128
FREQ = 256
MESH = pl.DeviceIdType.MESH
BF16 = jnp.bfloat16
F32 = jnp.float32


def time_embed(steps):
    half_width = FREQ // 2
    frequency = jnp.exp(-math.log(10000.0) * jnp.arange(half_width, dtype=F32) / half_width)
    angles = steps.astype(F32)[:, None] * frequency[None, :]
    return jnp.concatenate([jnp.cos(angles), jnp.sin(angles)], axis=1)


def split_feature(steps):
    feature = jax.nn.silu(time_embed(steps))
    high = lax.reduce_precision(feature, 8, 7)
    rest = feature - high
    mid = lax.reduce_precision(rest, 8, 7)
    low = rest - mid
    return jnp.concatenate([high, mid, low], axis=0).astype(BF16)


def kernel(
    target_ref, feat_ref, pairs_ref, mod_hbm, wqkv_hbm, wout_hbm,
    upd_ref,
    lat_ref, mod_v, mods, mod_send, mod_recv, hid_send,
    gath, w2, wo2, wn, wno, ws, wso,
    qkv, part, rf, rg, r1, r0,
    ld_sem, md_s, md_r, z_s, z_r, sw_s, sw_r, tok_s, tok_r, rs_s, rs_r,
):
    sections = lax.axis_size("section")
    tok = lat_ref.shape[1]
    depth = lat_ref.shape[2]
    latents = feat_ref.shape[0] // 3
    sec = lax.axis_index("section")
    tp = lax.axis_index("tp")
    core = lax.rem(sec, 2)
    x = tp // 4
    y = lax.rem(tp, 4)
    u = jnp.where(core == 0, y, x)
    v = jnp.where(core == 0, x, y)

    def at(uu, vv):
        return jnp.where(core == 0, vv * 4 + uu, uu * 4 + vv)

    def flip(a):
        return a + 1 - 2 * lax.rem(a, 2)

    pair = (sec, at(flip(u), v))
    p1 = (sec, at(3 - u, v))
    p2 = (sec, at(u, flip(v)))
    p3 = (sec, at(u, 3 - v))
    before = (lax.rem(sec + sections - 1, sections), tp)
    after = (lax.rem(sec + 1, sections), tp)
    is_a = (u == 0) | (u == 3)
    is_b = jnp.logical_not(is_a)
    prev = jnp.maximum(sec - 1, 0)
    first_moves = target_ref[2 * sec] != sec
    moved = first_moves | (target_ref[2 * sec + 1] != sec)
    prev_first = target_ref[2 * prev] != prev

    def remote(src, dst, ssem, rsem, peer):
        return pltpu.make_async_remote_copy(
            src_ref=src, dst_ref=dst, send_sem=ssem, recv_sem=rsem,
            device_id=peer, device_id_type=MESH,
        )

    own_lanes = pl.ds(0, HEAD_DIM)
    pair_lanes = pl.ds(HEAD_DIM, HEAD_DIM)
    mod_loads = [pltpu.make_async_copy(mod_hbm.at[c], mod_v.at[c], ld_sem.at[4 + c]) for c in range(3)]
    for load in mod_loads:
        load.start()

    barrier = pltpu.get_barrier_semaphore()
    for peer in (pair, p1, p2, p3, before, after):
        pl.semaphore_signal(barrier, inc=1, device_id=peer, device_id_type=MESH)
    pl.semaphore_wait(barrier, 6)

    z_copies = [
        remote(wqkv_hbm.at[i], wn.at[i], z_s.at[i], z_r.at[i], before) for i in range(1, 3)
    ]
    z_copies.append(remote(wout_hbm, wno, z_s.at[3], z_r.at[3], before))
    rows_half = wn.shape[1] // 2
    z_first = [
        remote(wqkv_hbm.at[0, rs], wn.at[0, rs], z_s.at[4 * k], z_r.at[4 * k], before)
        for k, rs in enumerate((pl.ds(0, rows_half), pl.ds(rows_half, rows_half)))
    ]

    def next_arrived(i):
        for copy in z_first if i == 0 else z_copies[i - 1 : i]:
            copy.wait_recv()

    direct = [
        remote(wqkv_hbm.at[i], w2.at[i, :, pair_lanes], sw_s.at[i], sw_r.at[i], pair)
        for i in range(3)
    ]
    direct.append(remote(wout_hbm, wo2.at[pair_lanes], sw_s.at[3], sw_r.at[3], pair))
    chosen = [
        remote(ws.at[i], w2.at[i, :, pair_lanes], sw_s.at[i], sw_r.at[i], pair)
        for i in range(3)
    ]
    chosen.append(remote(wso, wo2.at[pair_lanes], sw_s.at[3], sw_r.at[3], pair))
    z_first[0].start()

    @pl.when(is_b)
    def _():
        direct[0].start()

    loads = [
        pltpu.make_async_copy(wqkv_hbm.at[i], w2.at[i, :, own_lanes], ld_sem.at[i])
        for i in range(3)
    ]
    loads.append(pltpu.make_async_copy(wout_hbm, wo2.at[own_lanes], ld_sem.at[3]))
    loads[0].start()

    def select_weight(i, take_next, in_place):
        if i < 3:
            rows = w2.shape[1]
            step = min(512, rows)

            def piece(b, carry):
                rs = pl.ds(pl.multiple_of(b * step, step), step)
                picked = jnp.where(take_next, wn[i, rs, :], w2[i, rs, own_lanes])
                if in_place:
                    w2[i, rs, own_lanes] = picked
                else:
                    ws[i, rs, :] = picked
                return carry

            lax.fori_loop(0, rows // step, piece, 0)
        else:
            picked = jnp.where(take_next, wno[...], wo2[own_lanes, :])
            if in_place:
                wo2[own_lanes, :] = picked
            else:
                wso[...] = picked

    def send_weight(i, which):
        @pl.when(is_a & (core == which))
        def _():
            loads[i].wait()
            next_arrived(i)
            select_weight(i, moved, False)
            chosen[i].start()

    def make_mods(c):
        mod_loads[c].wait()
        prod = jnp.dot(feat_ref[...], mod_v[c], preferred_element_type=F32)
        mods[c] = prod[0:latents] + prod[latents : 2 * latents] + prod[2 * latents : 3 * latents]
        mod_send[c // 2, pl.ds(c % 2, 1), :] = jnp.where(
            prev_first, mods[c, pl.ds(2 * prev, 1), :], mods[c, pl.ds(2 * prev + 1, 1), :]
        )

    mod_send[...] = jnp.zeros_like(mod_send)
    md = [remote(mod_send.at[k], mod_recv.at[k], md_s.at[k], md_r.at[k], before) for k in range(2)]
    make_mods(0)
    make_mods(1)
    md[0].start()
    z_first[1].start()
    for copy in z_copies:
        copy.start()
    for load in loads[1:]:
        load.start()
    for k in range(2):
        lat_ref[k] = pairs_ref[:, k, :]

    def mod_row(c, moving):
        first = mods[c, pl.ds(2 * sec, 1), :]
        second = mods[c, pl.ds(2 * sec + 1, 1), :]
        if moving:
            arrived = mod_recv[c // 2, pl.ds(c % 2, 1), :]
            return jnp.where(moved, arrived, jnp.where(first_moves, first, second))
        return jnp.where(first_moves, second, first)

    def tokens(moving):
        if moving:
            return jnp.where(first_moves, lat_ref[0], lat_ref[1]).astype(F32)
        return jnp.where(first_moves, lat_ref[1], lat_ref[0]).astype(F32)

    def centre(moving):
        values = tokens(moving)
        centred = values - jnp.mean(values, axis=-1, keepdims=True)
        variance = jnp.mean(centred * centred, axis=-1, keepdims=True)
        return centred * lax.rsqrt(variance + 1e-06)

    def modulate(normed, moving):
        return (normed * (1.0 + mod_row(1, moving)) + mod_row(0, moving)).astype(BF16)

    cuts = 2
    piece_rows = tok // cuts

    def place(p):
        return gath.at[p // cuts, pl.ds((p % cuts) * piece_rows, piece_rows)]

    def doubling(slots_before, peer):
        count, first_sem = slots_before * cuts, (slots_before - 1) * cuts
        return [
            remote(place(p), place(count + p), tok_s.at[first_sem + p], tok_r.at[first_sem + p], peer)
            for p in range(count)
        ]

    t0 = [
        remote(hid_send.at[pl.ds(p * piece_rows, piece_rows)], place(cuts + p), tok_s.at[p], tok_r.at[p], pair)
        for p in range(cuts)
    ]
    d1, d2, d3 = doubling(2, p1), doubling(4, p2), doubling(8, p3)

    def pass_on(p):
        d3[p].start()
        if p < 4 * cuts:
            d2[p].start()
        if p < 2 * cuts:
            d1[p].start()

    stay_hidden = modulate(centre(False), False)

    @pl.when(is_a)
    def _():
        gath[0] = stay_hidden
        for p in range(cuts):
            pass_on(p)

    @pl.when(is_b)
    def _():
        hid_send[...] = stay_hidden
        for copy in t0:
            copy.start()

    send_weight(0, 0)
    md[0].wait_recv()
    move_hidden = modulate(centre(True), True)

    @pl.when(is_a)
    def _():
        hid_send[...] = move_hidden
        for copy in t0:
            copy.start()

    @pl.when(is_b)
    def _():
        gath[0] = move_hidden
        for p in range(cuts):
            pass_on(p)
        for i in range(1, 4):
            direct[i].start()

    make_mods(2)
    md[1].start()
    send_weight(1, 0)
    send_weight(0, 1)
    for p in range(cuts):
        t0[p].wait_recv()
        pass_on(cuts + p)
    send_weight(2, 0)
    for p in range(2 * cuts):
        d1[p].wait_recv()
        pass_on(2 * cuts + p)
    send_weight(3, 0)
    send_weight(1, 1)
    for p in range(2 * cuts):
        d2[p].wait_recv()
        pass_on(4 * cuts + p)
    send_weight(2, 1)
    for p in range(2 * cuts, 4 * cuts):
        d2[p].wait_recv()
        pass_on(4 * cuts + p)
    send_weight(3, 1)

    slots = 4
    width = slots * tok

    @pl.when(is_b)
    def _():
        for i in range(4):
            loads[i].wait()
            next_arrived(i)
            select_weight(i, moved, True)

    def project(i, b):
        rows = gath[pl.ds(b * slots, slots)].reshape(width, depth)
        out = jnp.dot(rows, w2[i], preferred_element_type=F32)
        qkv[i, pl.ds(b * width, width), :] = out.astype(BF16)

    for i in range(3):
        chosen[i].wait_recv()
        project(i, 0)
        project(i, 1)
    for b in (2, 3):
        for p in range(4 * cuts):
            d3[4 * cuts * (b - 2) + p].wait_recv()
        for i in range(3):
            project(i, b)
    chosen[3].wait_recv()

    half = depth // 2
    lanes_of = [pl.ds(0, half), pl.ds(half, half)]

    def low(j):
        return j if j < 4 else j - 4

    first, second, third, fourth = [{}, {}], [{}, {}], [{}, {}], []
    for h in range(2):
        lanes = lanes_of[h]
        jump = 8 - 4 * h
        goals = range(8) if h == 0 else (0, 1, 2, 3, 8, 9, 10, 11)

        def hop(src, dst, sem, peer):
            return remote(src, dst, rs_s.at[15 * h + sem], rs_r.at[15 * h + sem], peer)

        for n, j in enumerate(goals):
            first[h][j] = hop(part.at[j + jump, :, lanes], rf.at[h, n], n, (p3, p2)[h])
        for j in range(4):
            second[h][j] = hop(part.at[j + 12 - jump, :, lanes], rg.at[h, j], 8 + j, (p2, p3)[h])
        for j in range(2):
            third[h][j] = hop(part.at[j + 2, :, lanes], r1.at[j, :, lanes], 12 + j, p1)
        fourth.append(hop(part.at[1, :, lanes], r0.at[:, lanes], 14, pair))

    factor = HEAD_DIM ** (-0.5) * math.log2(math.e)
    n_col = 4
    col = depth // n_col

    def attend(b):
        rows = pl.ds(b * width, width)
        heads = []
        for h in range(2):
            lanes = pl.ds(h * HEAD_DIM, HEAD_DIM)
            scores = lax.dot_general(
                qkv[0, rows, lanes], qkv[1, :, lanes], (((1,), (1,)), ((), ())),
                preferred_element_type=F32,
            )
            top = jnp.max(scores, axis=-1, keepdims=True)
            weights = jnp.exp2((scores - top) * factor)
            total = jnp.sum(weights, axis=-1, keepdims=True)
            mixed = jnp.dot(weights.astype(BF16), qkv[2, :, lanes], preferred_element_type=F32)
            heads.append((mixed / total).astype(BF16))
        both = jnp.concatenate(heads, axis=1)
        for n in range(n_col):
            lanes = pl.ds(n * col, col)
            out = jnp.dot(both, wo2[:, lanes], preferred_element_type=F32).astype(BF16)
            part[pl.ds(b * slots, slots), :, lanes] = out.reshape(slots, tok, col)

    def begin(*goals):
        for h, j in goals:
            first[h][j].start()

    def second_stage(k):
        for h in range(2):
            j = k + 4 + 4 * h
            first[h][j].wait_recv()
            arrived = rf[h, j - 4 * h].astype(F32)
            part[j, :, lanes_of[h]] = (part[j, :, lanes_of[h]].astype(F32) + arrived).astype(BF16)
            second[h][k].start()

    def settle(k, h):
        first[h][k].wait_recv()
        second[h][k].wait_recv()
        own = part[k, :, lanes_of[h]].astype(F32)
        return own + rf[h, k].astype(F32) + rg[h, k].astype(F32)

    def third_stage(k):
        for h in range(2):
            part[k, :, lanes_of[h]] = settle(k, h).astype(BF16)
            third[h][k - 2].start()

    def finish(k, h):
        total = settle(k, h)
        third[h][k].wait_recv()
        return total + r1[k, :, lanes_of[h]].astype(F32)

    attend(3)
    begin((0, 7), (1, 11), (0, 5), (1, 9))
    attend(2)
    begin((0, 3), (0, 1))
    attend(1)
    begin((1, 3), (1, 1))
    attend(0)
    second_stage(3)
    second_stage(1)
    begin((0, 6), (1, 10), (0, 2), (1, 2), (0, 4), (1, 8), (0, 0), (1, 0))
    third_stage(3)
    second_stage(2)
    second_stage(0)
    for h in range(2):
        part[1, :, lanes_of[h]] = finish(1, h).astype(BF16)
        fourth[h].start()
    third_stage(2)
    keep = jnp.concatenate([finish(0, 0), finish(0, 1)], axis=1)
    md[1].wait_recv()
    for copy in fourth:
        copy.wait_recv()
    other = r0[...].astype(F32)
    stay_out = (tokens(False) + mod_row(2, False) * jnp.where(is_a, keep, other)).astype(BF16)
    move_out = (tokens(True) + mod_row(2, True) * jnp.where(is_a, other, keep)).astype(BF16)
    upd_ref[0] = jnp.where(first_moves, move_out, stay_out)
    upd_ref[1] = jnp.where(first_moves, stay_out, move_out)

    for copy in [*md, *z_first, *z_copies, *chosen, *t0, *d1, *d2, *d3, *fourth]:
        copy.wait_send()
    for group in (*first, *second, *third):
        for copy in group.values():
            copy.wait_send()


def body(latents, timestep, target, qkv_weight, mod_weight, out_weight):
    tok = latents.shape[0]
    depth = latents.shape[2]
    feature = split_feature(timestep)
    mod_table = jnp.transpose(mod_weight[0], (1, 0, 2))
    wqkv = jnp.transpose(qkv_weight[0], (1, 0, 2))
    wout = out_weight[0]
    vmem = pl.BlockSpec(memory_space=pltpu.VMEM)
    hbm = pl.BlockSpec(memory_space=pl.ANY)
    dma = pltpu.SemaphoreType.DMA
    updated = pl.pallas_call(
        kernel,
        out_shape=jax.ShapeDtypeStruct((2, tok, depth), BF16),
        in_specs=[pl.BlockSpec(memory_space=pltpu.SMEM), vmem, vmem, hbm, hbm, hbm],
        out_specs=vmem,
        scratch_shapes=[
            pltpu.VMEM((2, tok, depth), BF16),
            pltpu.VMEM(mod_table.shape, BF16),
            pltpu.VMEM((3, timestep.shape[0], depth), F32),
            pltpu.VMEM((2, 8, depth), F32),
            pltpu.VMEM((2, 8, depth), F32),
            pltpu.VMEM((tok, depth), BF16),
            pltpu.VMEM((16, tok, depth), BF16),
            pltpu.VMEM((3, depth, 2 * HEAD_DIM), BF16),
            pltpu.VMEM((2 * HEAD_DIM, depth), BF16),
            pltpu.VMEM((3, depth, HEAD_DIM), BF16),
            pltpu.VMEM((HEAD_DIM, depth), BF16),
            pltpu.VMEM((3, depth, HEAD_DIM), BF16),
            pltpu.VMEM((HEAD_DIM, depth), BF16),
            pltpu.VMEM((3, 16 * tok, 2 * HEAD_DIM), BF16),
            pltpu.VMEM((16, tok, depth), BF16),
            pltpu.VMEM((2, 8, tok, depth // 2), BF16),
            pltpu.VMEM((2, 4, tok, depth // 2), BF16),
            pltpu.VMEM((2, tok, depth), BF16),
            pltpu.VMEM((tok, depth), BF16),
            dma((7,)),
            dma((2,)),
            dma((2,)),
            dma((5,)),
            dma((5,)),
            dma((4,)),
            dma((4,)),
            dma((30,)),
            dma((30,)),
            dma((30,)),
            dma((30,)),
        ],
        compiler_params=pltpu.CompilerParams(
            collective_id=0, has_side_effects=True, vmem_limit_bytes=54 * 1024 * 1024
        ),
    )(target, feature, latents, mod_table, wqkv, wout)
    return jnp.transpose(updated, (1, 0, 2))


def solution(mesh):
    return jax.shard_map(
        body,
        mesh=mesh,
        in_specs=(
            P("tp", "section", None),
            P(),
            P(),
            P("section", None, None, "tp"),
            P("section", None, None, None),
            P("section", "tp", None),
        ),
        out_specs=P("tp", "section", None),
        check_vma=False,
    )
```

```python
import functools
import math

import jax
import jax.numpy as jnp
from jax import lax
from jax.experimental import pallas as pl
from jax.experimental.pallas import tpu as pltpu
from jax.sharding import PartitionSpec as P

HEAD_DIM = 128
FREQ = 256
MESH = pl.DeviceIdType.MESH
BF16 = jnp.bfloat16
F32 = jnp.float32


def time_embed(steps):
    half_width = FREQ // 2
    frequency = jnp.exp(-math.log(10000.0) * jnp.arange(half_width, dtype=F32) / half_width)
    angles = steps.astype(F32)[:, None] * frequency[None, :]
    return jnp.concatenate([jnp.cos(angles), jnp.sin(angles)], axis=1)


def split_feature(steps):
    feature = jax.nn.silu(time_embed(steps))
    high = lax.reduce_precision(feature, 8, 7)
    rest = feature - high
    mid = lax.reduce_precision(rest, 8, 7)
    low = rest - mid
    return jnp.concatenate([high, mid, low], axis=0).astype(BF16)


def kernel(
    target_ref, feat_ref, pairs_ref, mod_hbm, wqkv_hbm, wout_hbm,
    upd_ref,
    lat_ref, mod_v, mods, mod_send, mod_recv, hid_send,
    gath, w2, wo2, wn, wno, ws, wso,
    qkv, part, rf, rg, r1, r0,
    ld_sem, md_s, md_r, z_s, z_r, sw_s, sw_r, tok_s, tok_r, rs_s, rs_r,
):
    sections = lax.axis_size("section")
    tok = lat_ref.shape[1]
    depth = lat_ref.shape[2]
    latents = feat_ref.shape[0] // 3
    sec = lax.axis_index("section")
    tp = lax.axis_index("tp")
    core = lax.rem(sec, 2)
    x = tp // 4
    y = lax.rem(tp, 4)
    u = jnp.where(core == 0, y, x)
    v = jnp.where(core == 0, x, y)

    def at(uu, vv):
        return jnp.where(core == 0, vv * 4 + uu, uu * 4 + vv)

    def flip(a):
        return a + 1 - 2 * lax.rem(a, 2)

    pair = (sec, at(flip(u), v))
    p1 = (sec, at(3 - u, v))
    p2 = (sec, at(u, flip(v)))
    p3 = (sec, at(u, 3 - v))
    before = (lax.rem(sec + sections - 1, sections), tp)
    after = (lax.rem(sec + 1, sections), tp)
    is_a = (u == 0) | (u == 3)
    is_b = jnp.logical_not(is_a)
    prev = jnp.maximum(sec - 1, 0)
    first_moves = target_ref[2 * sec] != sec
    moved = first_moves | (target_ref[2 * sec + 1] != sec)
    prev_first = target_ref[2 * prev] != prev

    def remote(src, dst, ssem, rsem, peer):
        return pltpu.make_async_remote_copy(
            src_ref=src, dst_ref=dst, send_sem=ssem, recv_sem=rsem,
            device_id=peer, device_id_type=MESH,
        )

    own_lanes = pl.ds(0, HEAD_DIM)
    pair_lanes = pl.ds(HEAD_DIM, HEAD_DIM)
    mod_loads = [pltpu.make_async_copy(mod_hbm.at[c], mod_v.at[c], ld_sem.at[4 + c]) for c in range(3)]
    for load in mod_loads:
        load.start()

    barrier = pltpu.get_barrier_semaphore()
    for peer in (pair, p1, p2, p3, before, after):
        pl.semaphore_signal(barrier, inc=1, device_id=peer, device_id_type=MESH)
    pl.semaphore_wait(barrier, 6)

    z_copies = [
        remote(wqkv_hbm.at[i], wn.at[i], z_s.at[i], z_r.at[i], before) for i in range(1, 3)
    ]
    z_copies.append(remote(wout_hbm, wno, z_s.at[3], z_r.at[3], before))
    rows_half = wn.shape[1] // 2
    z_first = [
        remote(wqkv_hbm.at[0, rs], wn.at[0, rs], z_s.at[4 * k], z_r.at[4 * k], before)
        for k, rs in enumerate((pl.ds(0, rows_half), pl.ds(rows_half, rows_half)))
    ]

    def next_arrived(i):
        for copy in z_first if i == 0 else z_copies[i - 1 : i]:
            copy.wait_recv()

    direct = [
        remote(wqkv_hbm.at[i], w2.at[i, :, pair_lanes], sw_s.at[i], sw_r.at[i], pair)
        for i in range(3)
    ]
    direct.append(remote(wout_hbm, wo2.at[pair_lanes], sw_s.at[3], sw_r.at[3], pair))
    chosen = [
        remote(ws.at[i], w2.at[i, :, pair_lanes], sw_s.at[i], sw_r.at[i], pair)
        for i in range(3)
    ]
    chosen.append(remote(wso, wo2.at[pair_lanes], sw_s.at[3], sw_r.at[3], pair))
    z_first[0].start()

    @pl.when(is_b)
    def _():
        direct[0].start()

    loads = [
        pltpu.make_async_copy(wqkv_hbm.at[i], w2.at[i, :, own_lanes], ld_sem.at[i])
        for i in range(3)
    ]
    loads.append(pltpu.make_async_copy(wout_hbm, wo2.at[own_lanes], ld_sem.at[3]))
    loads[0].start()

    def select_weight(i, take_next, in_place):
        if i < 3:
            rows = w2.shape[1]
            step = min(512, rows)

            def piece(b, carry):
                rs = pl.ds(pl.multiple_of(b * step, step), step)
                picked = jnp.where(take_next, wn[i, rs, :], w2[i, rs, own_lanes])
                if in_place:
                    w2[i, rs, own_lanes] = picked
                else:
                    ws[i, rs, :] = picked
                return carry

            lax.fori_loop(0, rows // step, piece, 0)
        else:
            picked = jnp.where(take_next, wno[...], wo2[own_lanes, :])
            if in_place:
                wo2[own_lanes, :] = picked
            else:
                wso[...] = picked

    def send_weight(i, which):
        @pl.when(is_a & (core == which))
        def _():
            loads[i].wait()
            next_arrived(i)
            select_weight(i, moved, False)
            chosen[i].start()

    def make_mods(c):
        mod_loads[c].wait()
        prod = jnp.dot(feat_ref[...], mod_v[c], preferred_element_type=F32)
        mods[c] = prod[0:latents] + prod[latents : 2 * latents] + prod[2 * latents : 3 * latents]
        mod_send[c // 2, pl.ds(c % 2, 1), :] = jnp.where(
            prev_first, mods[c, pl.ds(2 * prev, 1), :], mods[c, pl.ds(2 * prev + 1, 1), :]
        )

    mod_send[...] = jnp.zeros_like(mod_send)
    md = [remote(mod_send.at[k], mod_recv.at[k], md_s.at[k], md_r.at[k], before) for k in range(2)]
    make_mods(0)
    make_mods(1)
    md[0].start()
    z_first[1].start()
    for copy in z_copies:
        copy.start()
    for load in loads[1:]:
        load.start()
    for k in range(2):
        lat_ref[k] = pairs_ref[:, k, :]

    def mod_row(c, moving):
        first = mods[c, pl.ds(2 * sec, 1), :]
        second = mods[c, pl.ds(2 * sec + 1, 1), :]
        if moving:
            arrived = mod_recv[c // 2, pl.ds(c % 2, 1), :]
            return jnp.where(moved, arrived, jnp.where(first_moves, first, second))
        return jnp.where(first_moves, second, first)

    def tokens(moving):
        if moving:
            return jnp.where(first_moves, lat_ref[0], lat_ref[1]).astype(F32)
        return jnp.where(first_moves, lat_ref[1], lat_ref[0]).astype(F32)

    def centre(moving):
        values = tokens(moving)
        centred = values - jnp.mean(values, axis=-1, keepdims=True)
        variance = jnp.mean(centred * centred, axis=-1, keepdims=True)
        return centred * lax.rsqrt(variance + 1e-06)

    def modulate(normed, moving):
        return (normed * (1.0 + mod_row(1, moving)) + mod_row(0, moving)).astype(BF16)

    cuts = 4
    piece_rows = tok // cuts

    def place(p):
        return gath.at[p // cuts, pl.ds((p % cuts) * piece_rows, piece_rows)]

    def doubling(slots_before, peer):
        count, first_sem = slots_before * cuts, (slots_before - 1) * cuts
        return [
            remote(place(p), place(count + p), tok_s.at[first_sem + p], tok_r.at[first_sem + p], peer)
            for p in range(count)
        ]

    t0 = [
        remote(hid_send.at[pl.ds(p * piece_rows, piece_rows)], place(cuts + p), tok_s.at[p], tok_r.at[p], pair)
        for p in range(cuts)
    ]
    d1, d2, d3 = doubling(2, p1), doubling(4, p2), doubling(8, p3)

    def pass_on(p):
        d3[p].start()
        if p < 4 * cuts:
            d2[p].start()
        if p < 2 * cuts:
            d1[p].start()

    stay_hidden = modulate(centre(False), False)

    @pl.when(is_a)
    def _():
        gath[0] = stay_hidden
        for p in range(cuts):
            pass_on(p)

    @pl.when(is_b)
    def _():
        hid_send[...] = stay_hidden
        for copy in t0:
            copy.start()

    send_weight(0, 0)
    md[0].wait_recv()
    move_hidden = modulate(centre(True), True)

    @pl.when(is_a)
    def _():
        hid_send[...] = move_hidden
        for copy in t0:
            copy.start()

    @pl.when(is_b)
    def _():
        gath[0] = move_hidden
        for p in range(cuts):
            pass_on(p)
        for i in range(1, 4):
            direct[i].start()

    make_mods(2)
    md[1].start()
    send_weight(1, 0)
    send_weight(0, 1)
    for p in range(cuts):
        t0[p].wait_recv()
        pass_on(cuts + p)
    send_weight(2, 0)
    for p in range(2 * cuts):
        d1[p].wait_recv()
        pass_on(2 * cuts + p)
    send_weight(3, 0)
    send_weight(1, 1)
    for p in range(2 * cuts):
        d2[p].wait_recv()
        pass_on(4 * cuts + p)
    send_weight(2, 1)
    for p in range(2 * cuts, 4 * cuts):
        d2[p].wait_recv()
        pass_on(4 * cuts + p)
    send_weight(3, 1)

    slots = 4
    width = slots * tok

    @pl.when(is_b)
    def _():
        for i in range(4):
            loads[i].wait()
            next_arrived(i)
            select_weight(i, moved, True)

    def project(i, b):
        rows = gath[pl.ds(b * slots, slots)].reshape(width, depth)
        out = jnp.dot(rows, w2[i], preferred_element_type=F32)
        qkv[i, pl.ds(b * width, width), :] = out.astype(BF16)

    for i in range(3):
        chosen[i].wait_recv()
        project(i, 0)
        project(i, 1)
    for b in (2, 3):
        for p in range(4 * cuts):
            d3[4 * cuts * (b - 2) + p].wait_recv()
        for i in range(3):
            project(i, b)
    chosen[3].wait_recv()

    half = depth // 2
    lanes_of = [pl.ds(0, half), pl.ds(half, half)]

    def low(j):
        return j if j < 4 else j - 4

    first, second, third, fourth = [{}, {}], [{}, {}], [{}, {}], []
    for h in range(2):
        lanes = lanes_of[h]
        jump = 8 - 4 * h
        goals = range(8) if h == 0 else (0, 1, 2, 3, 8, 9, 10, 11)

        def hop(src, dst, sem, peer):
            return remote(src, dst, rs_s.at[15 * h + sem], rs_r.at[15 * h + sem], peer)

        for n, j in enumerate(goals):
            first[h][j] = hop(part.at[j + jump, :, lanes], rf.at[h, n], n, (p3, p2)[h])
        for j in range(4):
            second[h][j] = hop(part.at[j + 12 - jump, :, lanes], rg.at[h, j], 8 + j, (p2, p3)[h])
        for j in range(2):
            third[h][j] = hop(part.at[j + 2, :, lanes], r1.at[j, :, lanes], 12 + j, p1)
        fourth.append(hop(part.at[1, :, lanes], r0.at[:, lanes], 14, pair))

    factor = HEAD_DIM ** (-0.5) * math.log2(math.e)
    n_col = 4
    col = depth // n_col

    def attend(b):
        rows = pl.ds(b * width, width)
        heads = []
        for h in range(2):
            lanes = pl.ds(h * HEAD_DIM, HEAD_DIM)
            scores = lax.dot_general(
                qkv[0, rows, lanes], qkv[1, :, lanes], (((1,), (1,)), ((), ())),
                preferred_element_type=F32,
            )
            top = jnp.max(scores, axis=-1, keepdims=True)
            weights = jnp.exp2((scores - top) * factor)
            total = jnp.sum(weights, axis=-1, keepdims=True)
            mixed = jnp.dot(weights.astype(BF16), qkv[2, :, lanes], preferred_element_type=F32)
            heads.append((mixed / total).astype(BF16))
        both = jnp.concatenate(heads, axis=1)
        for n in range(n_col):
            lanes = pl.ds(n * col, col)
            out = jnp.dot(both, wo2[:, lanes], preferred_element_type=F32).astype(BF16)
            part[pl.ds(b * slots, slots), :, lanes] = out.reshape(slots, tok, col)

    def begin(*goals):
        for h, j in goals:
            first[h][j].start()

    def second_stage(k):
        for h in range(2):
            j = k + 4 + 4 * h
            first[h][j].wait_recv()
            arrived = rf[h, j - 4 * h].astype(F32)
            part[j, :, lanes_of[h]] = (part[j, :, lanes_of[h]].astype(F32) + arrived).astype(BF16)
            second[h][k].start()

    def settle(k, h):
        first[h][k].wait_recv()
        second[h][k].wait_recv()
        own = part[k, :, lanes_of[h]].astype(F32)
        return own + rf[h, k].astype(F32) + rg[h, k].astype(F32)

    def third_stage(k):
        for h in range(2):
            part[k, :, lanes_of[h]] = settle(k, h).astype(BF16)
            third[h][k - 2].start()

    def finish(k, h):
        total = settle(k, h)
        third[h][k].wait_recv()
        return total + r1[k, :, lanes_of[h]].astype(F32)

    attend(3)
    begin((0, 7), (1, 11), (0, 5), (1, 9))
    attend(2)
    begin((0, 3), (0, 1))
    attend(1)
    begin((1, 3), (1, 1))
    attend(0)
    second_stage(3)
    second_stage(1)
    begin((0, 6), (1, 10), (0, 2), (1, 2), (0, 4), (1, 8), (0, 0), (1, 0))
    third_stage(3)
    second_stage(2)
    second_stage(0)
    for h in range(2):
        part[1, :, lanes_of[h]] = finish(1, h).astype(BF16)
        fourth[h].start()
    third_stage(2)
    keep = jnp.concatenate([finish(0, 0), finish(0, 1)], axis=1)
    md[1].wait_recv()
    for copy in fourth:
        copy.wait_recv()
    other = r0[...].astype(F32)
    stay_out = (tokens(False) + mod_row(2, False) * jnp.where(is_a, keep, other)).astype(BF16)
    move_out = (tokens(True) + mod_row(2, True) * jnp.where(is_a, other, keep)).astype(BF16)
    upd_ref[0] = jnp.where(first_moves, move_out, stay_out)
    upd_ref[1] = jnp.where(first_moves, stay_out, move_out)

    for copy in [*md, *z_first, *z_copies, *chosen, *t0, *d1, *d2, *d3, *fourth]:
        copy.wait_send()
    for group in (*first, *second, *third):
        for copy in group.values():
            copy.wait_send()


def body(latents, timestep, target, qkv_weight, mod_weight, out_weight):
    tok = latents.shape[0]
    depth = latents.shape[2]
    feature = split_feature(timestep)
    mod_table = jnp.transpose(mod_weight[0], (1, 0, 2))
    wqkv = jnp.transpose(qkv_weight[0], (1, 0, 2))
    wout = out_weight[0]
    vmem = pl.BlockSpec(memory_space=pltpu.VMEM)
    hbm = pl.BlockSpec(memory_space=pl.ANY)
    dma = pltpu.SemaphoreType.DMA
    updated = pl.pallas_call(
        kernel,
        out_shape=jax.ShapeDtypeStruct((2, tok, depth), BF16),
        in_specs=[pl.BlockSpec(memory_space=pltpu.SMEM), vmem, vmem, hbm, hbm, hbm],
        out_specs=vmem,
        scratch_shapes=[
            pltpu.VMEM((2, tok, depth), BF16),
            pltpu.VMEM(mod_table.shape, BF16),
            pltpu.VMEM((3, timestep.shape[0], depth), F32),
            pltpu.VMEM((2, 8, depth), F32),
            pltpu.VMEM((2, 8, depth), F32),
            pltpu.VMEM((tok, depth), BF16),
            pltpu.VMEM((16, tok, depth), BF16),
            pltpu.VMEM((3, depth, 2 * HEAD_DIM), BF16),
            pltpu.VMEM((2 * HEAD_DIM, depth), BF16),
            pltpu.VMEM((3, depth, HEAD_DIM), BF16),
            pltpu.VMEM((HEAD_DIM, depth), BF16),
            pltpu.VMEM((3, depth, HEAD_DIM), BF16),
            pltpu.VMEM((HEAD_DIM, depth), BF16),
            pltpu.VMEM((3, 16 * tok, 2 * HEAD_DIM), BF16),
            pltpu.VMEM((16, tok, depth), BF16),
            pltpu.VMEM((2, 8, tok, depth // 2), BF16),
            pltpu.VMEM((2, 4, tok, depth // 2), BF16),
            pltpu.VMEM((2, tok, depth), BF16),
            pltpu.VMEM((tok, depth), BF16),
            dma((7,)),
            dma((2,)),
            dma((2,)),
            dma((5,)),
            dma((5,)),
            dma((4,)),
            dma((4,)),
            dma((60,)),
            dma((60,)),
            dma((30,)),
            dma((30,)),
        ],
        compiler_params=pltpu.CompilerParams(
            collective_id=0, has_side_effects=True, vmem_limit_bytes=54 * 1024 * 1024
        ),
    )(target, feature, latents, mod_table, wqkv, wout)
    return jnp.transpose(updated, (1, 0, 2))


def solution(mesh):
    return jax.shard_map(
        body,
        mesh=mesh,
        in_specs=(
            P("tp", "section", None),
            P(),
            P(),
            P("section", None, None, "tp"),
            P("section", None, None, None),
            P("section", "tp", None),
        ),
        out_specs=P("tp", "section", None),
        check_vma=False,
    )
```
